32 devices in a mesh: seq: 4 (over y, x), batch: 8 (over z, core).
Axes of the slice: x: 2, y: 2, z: 4, core: 2. Of those that a mesh axis runs over, the one named last changes fastest.
Arguments:
- activations: bfloat16 [8, 3072, 4096], P('batch', 'seq'), may hold values from -18 to 18
- out_grads: bfloat16 [8, 3072, 4096], P('batch', 'seq'), may hold values from -0.29882812 to 0.29882812
- lengths: int32 [8, 3], P('batch'), may hold values from 1 to 1536, 3072 in all within a row
Outputs:
- act_factor: float32 [4096, 4096], P(('seq', 'batch'))
- grad_factor: float32 [4096, 4096], P(('seq', 'batch'))
The draws below stay inside these ranges and needn't reach their ends.
Inputs may be any that keep to these rules, and one draw needn't show every extreme that they name: `lengths`: each row sums to 3072 and its largest entry is exactly 1536.
All inputs are finite; a program needn't handle non-finite values.
Results may differ from the reference program's by a relative error of at most 0.004.
Values may be sent and summed in bfloat16 or wider, within the bound.
A program may use at most 64 MiB of HBM per device.

```python
import math
import jax
import jax.numpy as jnp
import numpy as np
from jax import lax

D = 4096
SEQS = 3
GROUP_TOK = 3072
MOST = 1536
GROUPS = 8
TOTAL_SEQS = 24


def with_spikes(values, stream_key, source, target, shards_of, factor):
    def block_of(dim):
        return (jnp.arange(values.shape[dim]) // (values.shape[dim] // shards_of)).reshape((-1,) + (1,) * (values.ndim - 1 - dim))

    one_side = jax.random.permutation(stream_key, shards_of)[block_of(target)]
    far = (block_of(target) + shards_of // 2) % shards_of
    return jnp.where((block_of(source) == one_side) | (block_of(source) == far), factor * values, values)


def shard_levels(own_key, extent, shards, least, high):
    def one(dim, shards_of):
        heights = jax.random.uniform(jax.random.fold_in(jax.random.fold_in(own_key, 6), dim), (shards_of,), jnp.float32, least / len(shards), high / len(shards))
        return jnp.repeat(jnp.exp(heights), extent[dim] // shards_of).reshape((-1,) + (1,) * (len(extent) - dim - 1))

    gain = one(*shards[0])
    for cut in shards[1:]:
        gain = gain * one(*cut)
    return gain


def split_up(count, total, reach, skew):
    weights = [(1 << 20) // math.isqrt(grade ** skew) + 1 for grade in range(2, count + 1)]
    rest, given = total - reach - (count - 1), [1] * (count - 1)
    while rest > 0:
        free = [i for i in range(count - 1) if given[i] < reach]
        mass, remaining = sum([weights[i] for i in free]), rest
        for i in free:
            more = min(reach - given[i], max(1, remaining * weights[i] // mass), rest)
            given[i] = given[i] + more
            rest = rest - more
    return np.array([reach] + given)


def uneven(key, number_of, total, reach, skew):
    if number_of == 2:
        one = jax.random.randint(key, (), max(1, total - reach), min(reach, total - 1) + 1)
        return jnp.stack([one, total - one])
    sizes = jnp.asarray(split_up(number_of, total, reach, skew), jnp.int32)
    twos = (number_of - 1) // 2
    source_of, taker = sizes[1:1 + 2 * twos:2], sizes[2:2 + 2 * twos:2]
    margin = jnp.minimum(source_of - 1, reach - taker)
    shifted = jax.random.randint(jax.random.fold_in(key, 1), (twos,), 0, 1 << 20) % (margin + 1)
    sizes = sizes.at[1:1 + 2 * twos:2].set(source_of - shifted).at[2:2 + 2 * twos:2].set(taker + shifted)
    return sizes[jax.random.permutation(jax.random.fold_in(key, 2), number_of)]


def bell_draw_with(stream_key, shape, width, most, split, heavy, held_as=jnp.bfloat16):
    array = width * jax.random.normal(stream_key, shape, jnp.float32)
    if split:
        array = array * shard_levels(stream_key, shape, split, -0.22, 0.18)
    return jnp.clip(with_spikes(array, jax.random.fold_in(stream_key, 3), *heavy), -most, most).astype(held_as)


def setup_inputs(seed: int = 0) -> dict:
    seeds = jax.random.split(jax.random.key(seed), 4)
    activations = bell_draw_with(seeds[0], (GROUPS, GROUP_TOK, D), 3.0, 18.0, ((0, 8), (1, 4)), (0, 2, 8, 2.0))
    out_grads = bell_draw_with(seeds[1], (GROUPS, GROUP_TOK, D), 0.05, 0.29882812, ((0, 8), (1, 4)), (0, 2, 8, 2.0))
    lengths = jax.vmap(lambda own: uneven(own, SEQS, GROUP_TOK, MOST, 2))(jax.random.split(seeds[2], GROUPS)).reshape((GROUPS, SEQS)).astype(jnp.int32)
    return dict(activations=activations, out_grads=out_grads, lengths=lengths)


def reference(activations, out_grads, lengths):
    ends = jnp.cumsum(lengths, axis=1).astype(jnp.int32)
    starts = ends - lengths
    position = jnp.arange(GROUP_TOK, dtype=jnp.int32)

    def reduce_group(item):
        act_group, grad_group, first, last = item
        member = (position[None, :] >= first[:, None]) & (position[None, :] < last[:, None])
        member = member.astype(jnp.bfloat16)
        act_sum = jnp.dot(member, act_group, preferred_element_type=jnp.float32)
        grad_sum = jnp.dot(member, grad_group, preferred_element_type=jnp.float32)
        return act_sum, grad_sum

    act_sum, grad_sum = lax.map(reduce_group, (activations, out_grads, starts, ends))
    act_rows = (act_sum / lengths[:, :, None].astype(jnp.float32)).astype(jnp.bfloat16).reshape(TOTAL_SEQS, D)
    grad_rows = grad_sum.astype(jnp.bfloat16).reshape(TOTAL_SEQS, D)
    act_factor = jnp.dot(act_rows.T, act_rows, preferred_element_type=jnp.float32) / TOTAL_SEQS
    grad_factor = jnp.dot(grad_rows.T, grad_rows, preferred_element_type=jnp.float32) / TOTAL_SEQS
    return act_factor, grad_factor
```

```python
import functools

import jax
import jax.numpy as jnp
from jax import lax
from jax.experimental import pallas as pl
from jax.experimental.pallas import tpu as pltpu
from jax.sharding import PartitionSpec as P

MESH = pl.DeviceIdType.MESH


def gather_kernel(S, B, count, len_ref, act_hbm, grad_hbm, gath, tokens, part, landed,
                  read_sem, rs_send, rs_recv, z_send, z_recv, p_send, p_recv, c_send, c_recv):
    Z = B // 2
    q = lax.axis_index("seq")
    b = lax.axis_index("batch")
    z, core = b // 2, b % 2
    T, D = act_hbm.shape[1:]
    cols = D // S
    R = part.shape[2]
    sources = (act_hbm, grad_hbm)
    order = tuple(range(1, S)) + (0,)

    def span(owner):
        return pl.ds(pl.multiple_of(owner * cols, cols), cols)

    def seq_at(k):
        return lax.rem(q + k, S)

    def z_at(j):
        return lax.rem(z + j, Z)

    def read(t, k):
        s = span(seq_at(k))
        return pltpu.make_async_copy(sources[t].at[0, :, s], tokens.at[t, :, s], read_sem.at[t, k])

    for t in range(2):
        for k in order:
            read(t, k).start()

    seq_peers = [{"seq": seq_at(k)} for k in range(1, S)]
    z_peers = [{"batch": z_at(j) * 2 + core} for j in range(1, Z)]
    other = {"batch": z * 2 + 1 - core}
    barrier = pltpu.get_barrier_semaphore()
    everyone = seq_peers + z_peers + [other]
    for peer in everyone:
        pl.semaphore_signal(barrier, inc=1, device_id=peer, device_id_type=MESH)

    row = lax.broadcasted_iota(jnp.int32, (8, T), 0)
    position = q * T + lax.broadcasted_iota(jnp.int32, (8, T), 1)
    first = jnp.zeros((8, T), jnp.int32)
    last = jnp.zeros((8, T), jnp.int32)
    begin = 0
    for s in range(count):
        end = begin + len_ref[0, s]
        first = jnp.where(row == s, begin, first)
        last = jnp.where(row == s, end, last)
        begin = end
    member = ((position >= first) & (position < last)).astype(jnp.float32).astype(jnp.bfloat16)

    which = lax.broadcasted_iota(jnp.int32, (R, cols), 0)
    sizes = jnp.ones((R, cols), jnp.float32)
    for s in range(count):
        sizes = jnp.where(which == s, len_ref[0, s].astype(jnp.float32), sizes)

    def scatter(t, k):
        return pltpu.make_async_remote_copy(
            src_ref=part.at[t, k], dst_ref=landed.at[t, k - 1],
            send_sem=rs_send.at[t, k - 1], recv_sem=rs_recv.at[t, k - 1],
            device_id=seq_peers[k - 1], device_id_type=MESH)

    def to_z(t, j):
        block = gath.at[t, core, z, :, span(q)]
        return pltpu.make_async_remote_copy(
            src_ref=block, dst_ref=block, send_sem=z_send.at[t, j - 1], recv_sem=z_recv.at[t, j - 1],
            device_id=z_peers[j - 1], device_id_type=MESH)

    def from_z(t, j):
        block = gath.at[t, core, z_at(Z - j), :, span(q)]
        return pltpu.make_async_remote_copy(
            src_ref=block, dst_ref=block, send_sem=z_send.at[t, j - 1], recv_sem=z_recv.at[t, j - 1],
            device_id=z_peers[j - 1], device_id_type=MESH)

    def to_plane(t, k, zz):
        block = gath.at[t, core, zz, :, span(q)]
        return pltpu.make_async_remote_copy(
            src_ref=block, dst_ref=block, send_sem=p_send.at[t, k - 1], recv_sem=p_recv.at[t, k - 1],
            device_id=seq_peers[k - 1], device_id_type=MESH)

    def plane_group(t, k, owner):
        block = gath.at[t, core, :, :, span(owner)]
        return pltpu.make_async_remote_copy(
            src_ref=block, dst_ref=block, send_sem=p_send.at[t, k - 1], recv_sem=p_recv.at[t, k - 1],
            device_id=seq_peers[k - 1], device_id_type=MESH)

    def to_core(t, k, side):
        block = gath.at[t, side, :, :, span(seq_at(S - k))]
        return pltpu.make_async_remote_copy(
            src_ref=block, dst_ref=block, send_sem=c_send.at[t, k], recv_sem=c_recv.at[t, k],
            device_id=other, device_id_type=MESH)

    for t in range(2):
        for k in order:
            read(t, k).wait()
            block = tokens[t, :, span(seq_at(k))]
            sums = jnp.dot(member, block, preferred_element_type=jnp.float32)
            part[t, k] = sums[:R]
            if t == 0 and k == order[0]:
                pl.semaphore_wait(barrier, len(everyone))
            if k:
                scatter(t, k).start()

    for t in range(2):
        total = part[t, 0]
        for k in range(1, S):
            scatter(t, k).wait_recv()
            total = total + landed[t, k - 1]
        if t == 0:
            total = total / sizes
        gath[t, core, z, :, span(q)] = total.astype(jnp.bfloat16)
        for j in range(1, Z):
            to_z(t, j).start()
        for k in range(1, S):
            to_plane(t, k, z).start()

    for t in range(2):
        for j in range(1, Z):
            from_z(t, j).wait_recv()
            for k in range(1, S):
                to_plane(t, k, z_at(Z - j)).start()
        to_core(t, 0, core).start()

    for t in range(2):
        for k in range(1, S):
            plane_group(t, k, seq_at(S - k)).wait_recv()
            to_core(t, k, core).start()

    for t in range(2):
        for k in range(S):
            to_core(t, k, 1 - core).wait_recv()
    for t in range(2):
        for k in range(S):
            to_core(t, k, core).wait_send()
        for k in range(1, S):
            scatter(t, k).wait_send()
            plane_group(t, k, q).wait_send()
        for j in range(1, Z):
            to_z(t, j).wait_send()


def outer_kernel(total, tile, steps, gath, act_out, grad_out, tiles, sem):
    D = gath.shape[-1]
    K = gath.shape[1] * gath.shape[2] * gath.shape[3]
    me = lax.axis_index("seq") * lax.axis_size("batch") + lax.axis_index("batch")
    at = me * tile
    width = D // steps
    outs = (act_out, grad_out)
    dims = (((0,), (0,)), ((), ()))
    wide = max(tile, 128)

    def rows(t, s):
        return gath[t, :, :, :, s].reshape(K, -1)

    def put(t, c):
        s = pl.ds(c * width, width)
        return pltpu.make_async_copy(tiles.at[t, :, s], outs[t].at[:, s], sem.at[t, c])

    for t in range(2):
        if tile % 128 == 0:
            mine = rows(t, pl.ds(pl.multiple_of(at, 128), tile))
        else:
            block = rows(t, pl.ds(pl.multiple_of(at // wide * wide, wide), wide))
            pick = lax.broadcasted_iota(jnp.int32, (wide, tile), 0) == at % wide + lax.broadcasted_iota(jnp.int32, (wide, tile), 1)
            mine = jnp.dot(block, pick.astype(jnp.float32).astype(jnp.bfloat16), preferred_element_type=jnp.float32).astype(jnp.bfloat16)
        for c in range(steps):
            s = pl.ds(c * width, width)
            new = lax.dot_general(mine, rows(t, s), dims, preferred_element_type=jnp.float32)
            tiles[t, :, s] = new * (1.0 / total)
            put(t, c).start()
    for t in range(2):
        for c in range(steps):
            put(t, c).wait()


def solution(mesh):
    S, B = mesh.shape["seq"], mesh.shape["batch"]
    Z = B // 2

    def local(activations, out_grads, lengths):
        T, D = activations.shape[1:]
        count = lengths.shape[1]
        R = max(2, 1 << (count - 1).bit_length())
        cols = D // S
        tile = D // (S * B)
        steps = 4
        gath = pl.pallas_call(
            functools.partial(gather_kernel, S, B, count),
            out_shape=jax.ShapeDtypeStruct((2, 2, Z, R, D), jnp.bfloat16),
            in_specs=[pl.BlockSpec(memory_space=pltpu.SMEM), pl.BlockSpec(memory_space=pl.ANY), pl.BlockSpec(memory_space=pl.ANY)],
            out_specs=pl.BlockSpec(memory_space=pltpu.VMEM),
            scratch_shapes=[
                pltpu.VMEM((2, T, D), jnp.bfloat16),
                pltpu.VMEM((2, S, R, cols), jnp.float32),
                pltpu.VMEM((2, S - 1, R, cols), jnp.float32),
                pltpu.SemaphoreType.DMA((2, S)),
                pltpu.SemaphoreType.DMA((2, S - 1)),
                pltpu.SemaphoreType.DMA((2, S - 1)),
                pltpu.SemaphoreType.DMA((2, Z - 1)),
                pltpu.SemaphoreType.DMA((2, Z - 1)),
                pltpu.SemaphoreType.DMA((2, S - 1)),
                pltpu.SemaphoreType.DMA((2, S - 1)),
                pltpu.SemaphoreType.DMA((2, S)),
                pltpu.SemaphoreType.DMA((2, S)),
            ],
            compiler_params=pltpu.CompilerParams(collective_id=0, has_side_effects=True),
            name="gather_rows",
        )(lengths, activations, out_grads)
        out = jax.ShapeDtypeStruct((tile, D), jnp.float32)
        return tuple(pl.pallas_call(
            functools.partial(outer_kernel, count * B, tile, steps),
            out_shape=(out, out),
            in_specs=[pl.BlockSpec(memory_space=pltpu.VMEM)],
            out_specs=(pl.BlockSpec(memory_space=pl.ANY), pl.BlockSpec(memory_space=pl.ANY)),
            scratch_shapes=[pltpu.VMEM((2, tile, D), jnp.float32), pltpu.SemaphoreType.DMA((2, steps))],
            name="outer_rows",
        )(gath))

    in_specs = (P("batch", "seq", None), P("batch", "seq", None), P("batch", None))
    out_specs = (P(("seq", "batch"), None), P(("seq", "batch"), None))
    return jax.shard_map(local, mesh=mesh, in_specs=in_specs, out_specs=out_specs, check_vma=False)
```

```python
import functools

import jax
import jax.numpy as jnp
from jax import lax
from jax.experimental import pallas as pl
from jax.experimental.pallas import tpu as pltpu
from jax.sharding import PartitionSpec as P

MESH = pl.DeviceIdType.MESH


def factor_kernel(S, B, H, count, len_ref, act_hbm, grad_hbm, act_tile, grad_tile, gath, tokens, part, landed,
                  read_sem, rs_send, rs_recv, z_send, z_recv, p_send, p_recv, c_send, c_recv):
    Z = B // 2
    q = lax.axis_index("seq")
    b = lax.axis_index("batch")
    z, core = b // 2, b % 2
    T, D = act_hbm.shape[1:]
    cols = D // S
    width = cols // H
    R = part.shape[2]
    sources = (act_hbm, grad_hbm)
    tiles = (act_tile, grad_tile)
    tile = act_tile.shape[0]
    order = tuple(range(1, S)) + (0,)
    units = [(t, h) for t in range(2) for h in range(H)]

    def span(owner, h):
        return pl.ds(pl.multiple_of(owner * cols + h * width, width), width)

    def seq_at(k):
        return lax.rem(q + k, S)

    def z_at(j):
        return lax.rem(z + j, Z)

    def read(u, k):
        t, h = units[u]
        s = span(seq_at(k), h)
        return pltpu.make_async_copy(sources[t].at[0, :, s], tokens.at[t, :, s], read_sem.at[u, k])

    for u in range(len(units)):
        for k in order:
            read(u, k).start()

    seq_peers = [{"seq": seq_at(k)} for k in range(1, S)]
    z_peers = [{"batch": z_at(j) * 2 + core} for j in range(1, Z)]
    other = {"batch": z * 2 + 1 - core}
    barrier = pltpu.get_barrier_semaphore()
    everyone = seq_peers + z_peers + [other]
    for peer in everyone:
        pl.semaphore_signal(barrier, inc=1, device_id=peer, device_id_type=MESH)

    row = lax.broadcasted_iota(jnp.int32, (8, T), 0)
    position = q * T + lax.broadcasted_iota(jnp.int32, (8, T), 1)
    first = jnp.zeros((8, T), jnp.int32)
    last = jnp.zeros((8, T), jnp.int32)
    begin = 0
    for s in range(count):
        end = begin + len_ref[0, s]
        first = jnp.where(row == s, begin, first)
        last = jnp.where(row == s, end, last)
        begin = end
    member = ((position >= first) & (position < last)).astype(jnp.float32).astype(jnp.bfloat16)

    which = lax.broadcasted_iota(jnp.int32, (R, width), 0)
    sizes = jnp.ones((R, width), jnp.float32)
    for s in range(count):
        sizes = jnp.where(which == s, len_ref[0, s].astype(jnp.float32), sizes)

    def send(src, dst, send_sem, recv_sem, peer):
        return pltpu.make_async_remote_copy(
            src_ref=src, dst_ref=dst, send_sem=send_sem, recv_sem=recv_sem, device_id=peer, device_id_type=MESH)

    def scatter(u, k):
        return send(part.at[u, k], landed.at[u, k - 1], rs_send.at[u, k - 1], rs_recv.at[u, k - 1], seq_peers[k - 1])

    def at_z(u, j, zz):
        t, h = units[u]
        block = gath.at[t, core, zz, :, span(q, h)]
        return send(block, block, z_send.at[u, j - 1], z_recv.at[u, j - 1], z_peers[j - 1])

    def to_plane(u, k, zz):
        t, h = units[u]
        block = gath.at[t, core, zz, :, span(q, h)]
        return send(block, block, p_send.at[u, k - 1], p_recv.at[u, k - 1], seq_peers[k - 1])

    def plane_group(u, k, owner):
        t, h = units[u]
        block = gath.at[t, core, :, :, span(owner, h)]
        return send(block, block, p_send.at[u, k - 1], p_recv.at[u, k - 1], seq_peers[k - 1])

    def to_core(u, k, side):
        t, h = units[u]
        block = gath.at[t, side, :, :, span(seq_at(S - k), h)]
        return send(block, block, c_send.at[u, k], c_recv.at[u, k], other)

    for u, (t, h) in enumerate(units):
        for k in order:
            read(u, k).wait()
            sums = jnp.dot(member, tokens[t, :, span(seq_at(k), h)], preferred_element_type=jnp.float32)
            part[u, k] = sums[:R]
            if u == 0 and k == order[0]:
                pl.semaphore_wait(barrier, len(everyone))
            if k:
                scatter(u, k).start()

    for u, (t, h) in enumerate(units):
        total = part[u, 0]
        for k in range(1, S):
            scatter(u, k).wait_recv()
            total = total + landed[u, k - 1]
        if t == 0:
            total = total / sizes
        gath[t, core, z, :, span(q, h)] = total.astype(jnp.bfloat16)
        for j in range(1, Z):
            at_z(u, j, z).start()
        for k in range(1, S):
            to_plane(u, k, z).start()

    for u in range(len(units)):
        for j in range(1, Z):
            at_z(u, j, z_at(Z - j)).wait_recv()
            for k in range(1, S):
                to_plane(u, k, z_at(Z - j)).start()
        to_core(u, 0, core).start()

    K = gath.shape[1] * Z * R

    def rows(t, s):
        return gath[t, :, :, :, s].reshape(K, -1)

    wide = max(tile, 128)
    at = q * cols + b * tile

    for t in range(2):
        mine = [u for u in range(len(units)) if units[u][0] == t]
        for u in mine:
            for k in range(1, S):
                plane_group(u, k, seq_at(S - k)).wait_recv()
                to_core(u, k, core).start()
        for u in mine:
            to_core(u, 0, 1 - core).wait_recv()
        if tile % 128 == 0:
            block = rows(t, pl.ds(pl.multiple_of(at, 128), tile))
        else:
            block = rows(t, pl.ds(pl.multiple_of(at // wide * wide, wide), wide))
            pick = lax.broadcasted_iota(jnp.int32, (wide, tile), 0) == at % wide + lax.broadcasted_iota(jnp.int32, (wide, tile), 1)
            block = jnp.dot(block, pick.astype(jnp.float32).astype(jnp.bfloat16), preferred_element_type=jnp.float32).astype(jnp.bfloat16)
        left = block.T
        for u in mine:
            h = units[u][1]
            for k in range(S):
                if k:
                    to_core(u, k, 1 - core).wait_recv()
                s = span(seq_at(S - k), h)
                tiles[t][:, s] = jnp.dot(left, rows(t, s), preferred_element_type=jnp.float32) * (1.0 / (count * B))

    for u in range(len(units)):
        for k in range(S):
            to_core(u, k, core).wait_send()
        for k in range(1, S):
            scatter(u, k).wait_send()
            plane_group(u, k, q).wait_send()
        for j in range(1, Z):
            at_z(u, j, z).wait_send()


def solution(mesh):
    S, B = mesh.shape["seq"], mesh.shape["batch"]
    Z = B // 2

    def local(activations, out_grads, lengths):
        T, D = activations.shape[1:]
        count = lengths.shape[1]
        R = max(2, 1 << (count - 1).bit_length())
        cols = D // S
        tile = D // (S * B)
        H = 2
        U = 2 * H
        out = pltpu.VMEM((tile, D), jnp.float32)
        return tuple(pl.pallas_call(
            functools.partial(factor_kernel, S, B, H, count),
            out_shape=(out, out),
            in_specs=[pl.BlockSpec(memory_space=pltpu.SMEM), pl.BlockSpec(memory_space=pl.ANY), pl.BlockSpec(memory_space=pl.ANY)],
            out_specs=(pl.BlockSpec(memory_space=pltpu.VMEM), pl.BlockSpec(memory_space=pltpu.VMEM)),
            scratch_shapes=[
                pltpu.VMEM((2, 2, Z, R, D), jnp.bfloat16),
                pltpu.VMEM((2, T, D), jnp.bfloat16),
                pltpu.VMEM((U, S, R, cols // H), jnp.float32),
                pltpu.VMEM((U, S - 1, R, cols // H), jnp.float32),
                pltpu.SemaphoreType.DMA((U, S)),
                pltpu.SemaphoreType.DMA((U, S - 1)),
                pltpu.SemaphoreType.DMA((U, S - 1)),
                pltpu.SemaphoreType.DMA((U, Z - 1)),
                pltpu.SemaphoreType.DMA((U, Z - 1)),
                pltpu.SemaphoreType.DMA((U, S - 1)),
                pltpu.SemaphoreType.DMA((U, S - 1)),
                pltpu.SemaphoreType.DMA((U, S)),
                pltpu.SemaphoreType.DMA((U, S)),
            ],
            compiler_params=pltpu.CompilerParams(collective_id=0, has_side_effects=True, vmem_limit_bytes=56 * 2**20),
            name="factors",
        )(lengths, activations, out_grads))

    in_specs = (P("batch", "seq", None), P("batch", "seq", None), P("batch", None))
    out_specs = (P(("seq", "batch"), None), P(("seq", "batch"), None))
    return jax.shard_map(local, mesh=mesh, in_specs=in_specs, out_specs=out_specs, check_vma=False)
```

```python
import functools

import jax
import jax.numpy as jnp
from jax import lax
from jax.experimental import pallas as pl
from jax.experimental.pallas import tpu as pltpu
from jax.sharding import PartitionSpec as P

MESH = pl.DeviceIdType.MESH


def factor_kernel(S, B, units, count, len_ref, act_hbm, grad_hbm, act_tile, grad_tile, gath, tokens, part, landed,
                  read_sem, rs_send, rs_recv, z_send, z_recv, p_send, p_recv, c_send, c_recv):
    Z = B // 2
    q = lax.axis_index("seq")
    b = lax.axis_index("batch")
    z, core = b // 2, b % 2
    T, D = act_hbm.shape[1:]
    cols = D // S
    R = part.shape[2]
    sources = (act_hbm, grad_hbm)
    tiles = (act_tile, grad_tile)
    tile = act_tile.shape[0]
    U = len(units)

    def read(u, c):
        t, low, width = units[u]
        s = pl.ds(c * cols + low, width)
        return pltpu.make_async_copy(sources[t].at[0, :, s], tokens.at[t, :, s], read_sem.at[u, c])

    for u in range(U):
        for c in range(S):
            read(u, c).start()

    def seq_at(k):
        return lax.rem(q + k, S)

    def z_at(j):
        return lax.rem(z + j, Z)

    def span(owner, u):
        t, low, width = units[u]
        return pl.ds(pl.multiple_of(owner * cols + low, 128), width)

    def within(u):
        return pl.ds(units[u][1], units[u][2])

    seq_peers = [{"seq": seq_at(k)} for k in range(1, S)]
    z_peers = [{"batch": z_at(j) * 2 + core} for j in range(1, Z)]
    other = {"batch": z * 2 + 1 - core}
    barrier = pltpu.get_barrier_semaphore()
    everyone = seq_peers + z_peers + [other]
    for peer in everyone:
        pl.semaphore_signal(barrier, inc=1, device_id=peer, device_id_type=MESH)

    row = lax.broadcasted_iota(jnp.int32, (8, T), 0)
    position = q * T + lax.broadcasted_iota(jnp.int32, (8, T), 1)
    first = jnp.zeros((8, T), jnp.int32)
    last = jnp.zeros((8, T), jnp.int32)
    begin = 0
    for s in range(count):
        end = begin + len_ref[0, s]
        first = jnp.where(row == s, begin, first)
        last = jnp.where(row == s, end, last)
        begin = end
    member = ((position >= first) & (position < last)).astype(jnp.float32).astype(jnp.bfloat16)

    which = lax.broadcasted_iota(jnp.int32, (R, cols), 0)
    sizes = jnp.ones((R, cols), jnp.float32)
    for s in range(count):
        sizes = jnp.where(which == s, len_ref[0, s].astype(jnp.float32), sizes)

    def send(src, dst, send_sem, recv_sem, peer):
        return pltpu.make_async_remote_copy(
            src_ref=src, dst_ref=dst, send_sem=send_sem, recv_sem=recv_sem, device_id=peer, device_id_type=MESH)

    def scatter(u, k):
        t = units[u][0]
        return send(part.at[t, seq_at(k), :, within(u)], landed.at[t, k - 1, :, within(u)],
                    rs_send.at[u, k - 1], rs_recv.at[u, k - 1], seq_peers[k - 1])

    def scatter_to(u, c):
        t = units[u][0]
        slot = lax.rem(c - q + S, S) - 1

        @pl.when(q != c)
        def _():
            send(part.at[t, c, :, within(u)], landed.at[t, slot, :, within(u)],
                 rs_send.at[u, slot], rs_recv.at[u, slot], {"seq": jnp.int32(c)}).start()

    def at_z(u, j, zz):
        block = gath.at[units[u][0], core, zz, :, span(q, u)]
        return send(block, block, z_send.at[u, j - 1], z_recv.at[u, j - 1], z_peers[j - 1])

    def to_plane(u, k, zz):
        block = gath.at[units[u][0], core, zz, :, span(q, u)]
        return send(block, block, p_send.at[u, k - 1], p_recv.at[u, k - 1], seq_peers[k - 1])

    def plane_group(u, k, owner):
        block = gath.at[units[u][0], core, :, :, span(owner, u)]
        return send(block, block, p_send.at[u, k - 1], p_recv.at[u, k - 1], seq_peers[k - 1])

    def to_core(u, k, side):
        block = gath.at[units[u][0], side, :, :, span(seq_at(S - k), u)]
        return send(block, block, c_send.at[u, k], c_recv.at[u, k], other)

    for u, (t, low, width) in enumerate(units):
        for c in range(S):
            read(u, c).wait()
            block = tokens[t, :, c * cols + low:c * cols + low + width]
            sums = jnp.dot(member, block, preferred_element_type=jnp.float32)[:R]
            part[t, c, :, low:low + width] = sums / sizes[:, :width] if t == 0 else sums
            if u == 0 and c == 0:
                pl.semaphore_wait(barrier, len(everyone))
            scatter_to(u, c)

    for u, (t, low, width) in enumerate(units):
        total = part[t, q, :, low:low + width]
        for k in range(1, S):
            scatter(u, k).wait_recv()
            total = total + landed[t, k - 1, :, low:low + width]
        gath[t, core, z, :, span(q, u)] = total.astype(jnp.bfloat16)
        for j in range(1, Z):
            at_z(u, j, z).start()
        for k in range(1, S):
            to_plane(u, k, z).start()

    for u in range(U):
        for j in range(1, Z):
            at_z(u, j, z_at(Z - j)).wait_recv()
            for k in range(1, S):
                to_plane(u, k, z_at(Z - j)).start()
        to_core(u, 0, core).start()

    K = 2 * Z * R

    def rows(t, s):
        return gath[t, :, :, :, s].reshape(K, -1)

    wide = max(tile, 128)
    at = q * cols + b * tile

    for t in range(2):
        mine = [u for u in range(U) if units[u][0] == t]

        for u in mine:
            for k in range(1, S):
                plane_group(u, k, seq_at(S - k)).wait_recv()
                to_core(u, k, core).start()
        for u in mine:
            for k in range(S):
                to_core(u, k, 1 - core).wait_recv()

        if tile % 128 == 0:
            block = rows(t, pl.ds(pl.multiple_of(at, 128), tile))
        else:
            block = rows(t, pl.ds(pl.multiple_of(at // wide * wide, wide), wide))
            pick = lax.broadcasted_iota(jnp.int32, (wide, tile), 0) == at % wide + lax.broadcasted_iota(jnp.int32, (wide, tile), 1)
            block = jnp.dot(block, pick.astype(jnp.float32).astype(jnp.bfloat16), preferred_element_type=jnp.float32).astype(jnp.bfloat16)
        left = block.T
        for c in range(S):
            s = slice(c * cols, (c + 1) * cols)
            tiles[t][:, s] = jnp.dot(left, rows(t, s), preferred_element_type=jnp.float32) * (1.0 / (count * B))

    for u in range(U):
        for k in range(S):
            to_core(u, k, core).wait_send()
        for k in range(1, S):
            plane_group(u, k, q).wait_send()
            scatter(u, k).wait_send()
        for j in range(1, Z):
            at_z(u, j, z).wait_send()


def put_kernel(steps, act_tile, grad_tile, act_out, grad_out, sem):
    step = act_tile.shape[1] // steps
    copies = [pltpu.make_async_copy(src.at[:, pl.ds(i * step, step)], dst.at[:, pl.ds(i * step, step)], sem.at[t, i])
              for t, (src, dst) in enumerate(((act_tile, act_out), (grad_tile, grad_out))) for i in range(steps)]
    for copy in copies:
        copy.start()
    for copy in copies:
        copy.wait()


def solution(mesh):
    S, B = mesh.shape["seq"], mesh.shape["batch"]
    Z = B // 2

    def local(activations, out_grads, lengths):
        T, D = activations.shape[1:]
        count = lengths.shape[1]
        R = max(2, 1 << (count - 1).bit_length())
        cols = D // S
        tile = D // (S * B)
        half = cols // 2
        units = ((0, 0, cols), (1, 0, half), (1, half, half))
        U = len(units)
        out = pltpu.VMEM((tile, D), jnp.float32)
        tiles = pl.pallas_call(
            functools.partial(factor_kernel, S, B, units, count),
            out_shape=(out, out),
            in_specs=[pl.BlockSpec(memory_space=pltpu.SMEM), pl.BlockSpec(memory_space=pl.ANY), pl.BlockSpec(memory_space=pl.ANY)],
            out_specs=(pl.BlockSpec(memory_space=pltpu.VMEM), pl.BlockSpec(memory_space=pltpu.VMEM)),
            scratch_shapes=[
                pltpu.VMEM((2, 2, Z, R, D), jnp.bfloat16),
                pltpu.VMEM((2, T, D), jnp.bfloat16),
                pltpu.VMEM((2, S, R, cols), jnp.float32),
                pltpu.VMEM((2, S - 1, R, cols), jnp.float32),
                pltpu.SemaphoreType.DMA((U, S)),
                pltpu.SemaphoreType.DMA((U, S - 1)),
                pltpu.SemaphoreType.DMA((U, S - 1)),
                pltpu.SemaphoreType.DMA((U, Z - 1)),
                pltpu.SemaphoreType.DMA((U, Z - 1)),
                pltpu.SemaphoreType.DMA((U, S - 1)),
                pltpu.SemaphoreType.DMA((U, S - 1)),
                pltpu.SemaphoreType.DMA((U, S)),
                pltpu.SemaphoreType.DMA((U, S)),
            ],
            compiler_params=pltpu.CompilerParams(collective_id=0, has_side_effects=True, vmem_limit_bytes=56 * 2**20),
            name="factors",
        )(lengths, activations, out_grads)
        steps = 4
        held = jax.ShapeDtypeStruct((tile, D), jnp.float32)
        return tuple(pl.pallas_call(
            functools.partial(put_kernel, steps),
            out_shape=(held, held),
            in_specs=[pl.BlockSpec(memory_space=pltpu.VMEM)] * 2,
            out_specs=(pl.BlockSpec(memory_space=pl.ANY), pl.BlockSpec(memory_space=pl.ANY)),
            scratch_shapes=[pltpu.SemaphoreType.DMA((2, steps))],
            compiler_params=pltpu.CompilerParams(vmem_limit_bytes=16 * 2**20),
            name="put_tiles",
        )(*tiles))

    in_specs = (P("batch", "seq", None), P("batch", "seq", None), P("batch", None))
    out_specs = (P(("seq", "batch"), None), P(("seq", "batch"), None))
    return jax.shard_map(local, mesh=mesh, in_specs=in_specs, out_specs=out_specs, check_vma=False)
```
